256 devices in a mesh: expert: 64 (over x, z, core), mp: 4 (over y).
Axes of the slice: x: 4, y: 4, z: 8, core: 2. Of those that a mesh axis runs over, the one named last changes fastest.
Arguments:
- tokens: bfloat16 [1536, 6144], P('expert', 'mp'), may hold values from -6 to 6
- mix_weights: float32 [1536, 2], P('expert'), may hold values from 0.2 to 1
- routes: int32 [1536, 2], P('expert'), may hold values from 0 to 7, as said below
- w_gate: bfloat16 [64, 6144, 1024], P('expert', None, 'mp'), may hold values from -0.078125 to 0.078125
- w_up: bfloat16 [64, 6144, 1024], P('expert', None, 'mp'), may hold values from -0.078125 to 0.078125
- w_down: bfloat16 [64, 1024, 6144], P('expert', 'mp'), may hold values from -0.0625 to 0.0625
Outputs:
- mixed_out: bfloat16 [1536, 6144], P('expert', 'mp')
The draws below stay inside these ranges and needn't reach their ends.
Inputs may be any that keep to these rules, and one draw needn't show every extreme that they name: `routes`: each row names 2 different experts, and every expert is named by some row. Among the 24 rows of one index of the expert axis no expert is named more than 12 times, and on some indices one is named exactly 12 times.
All inputs are finite; a program needn't handle non-finite values.
Results may differ from the reference program's by a relative error of at most 0.011.
Values may be sent and summed in bfloat16 or wider, within the bound.
No kernel may reach another device: no remote copies, remote signals or barrier semaphores. Data moves between devices by JAX's collectives and lax.ppermute only.
A program may use at most 128 MiB of HBM per device.

```python
import jax
import jax.numpy as jnp

D = 6144
FF = 8192
EXPERTS = 8
TOP = 2
TOK_DEV = 24
MOST = 12
GROUP = 8
FF_SLICE = 1024
TOKENS = 1536
CAP = 480


def block_routes(block_key, busiest):
    order_key, rows_key, shift_key = jax.random.split(block_key, 3)
    others_order = jax.random.permutation(order_key, EXPERTS - 1).astype(jnp.int32)
    others = ((busiest + 1 + others_order) % EXPERTS).astype(jnp.int32)
    row_order = jax.random.permutation(rows_key, TOK_DEV).astype(jnp.int32)
    shift = jax.random.randint(shift_key, (), 0, EXPERTS - 2).astype(jnp.int32)
    first = jnp.where(row_order < MOST, busiest, others[0]).astype(jnp.int32)
    second_idx = (1 + (row_order + shift) % (EXPERTS - 2)).astype(jnp.int32)
    second = jnp.take(others, second_idx).astype(jnp.int32)
    return jnp.stack([first, second], axis=1).astype(jnp.int32)


def draw_routes(key, part):
    base = jax.random.fold_in(key, 4711)
    busiest = jax.random.randint(jax.random.fold_in(base, 99), (), 0, EXPERTS).astype(jnp.int32)
    block_count = TOKENS // TOK_DEV
    keys = jax.random.split(base, block_count)
    grids = jax.vmap(block_routes, in_axes=(0, None))(keys, busiest)
    return grids.reshape(TOKENS, TOP).astype(jnp.int32)


def level_of(stream_key, dims, cuts, least, largest):
    factor_of = 1.0
    for axis_at, shards_of in cuts:
        heights = jax.random.uniform(jax.random.fold_in(jax.random.fold_in(stream_key, 6), axis_at), (shards_of,), jnp.float32, least / len(cuts), largest / len(cuts))
        factor_of = factor_of * jnp.repeat(jnp.exp(heights), dims[axis_at] // shards_of).reshape((-1,) + (1,) * (len(dims) - 1 - axis_at))
    return factor_of


def bell_draw(stream_key, extent, deviation, bound, shards=(), kind=jnp.bfloat16):
    result = deviation * jax.random.normal(stream_key, extent, jnp.float32)
    if shards:
        result = result * level_of(stream_key, extent, shards, -0.22, 0.18)
    return jnp.clip(result, -bound, bound).astype(kind)


def setup_inputs(seed: int = 0) -> dict:
    streams_of = jax.random.split(jax.random.key(seed), 7)
    return {
        "tokens": bell_draw(streams_of[0], (TOKENS, D), 1.0, 6.0, ((0, 64), (1, 4))),
        "mix_weights": jnp.clip(0.2 + 0.8 * jax.random.uniform(streams_of[1], (TOKENS, TOP), jnp.float32) ** level_of(streams_of[1], (TOKENS, TOP), ((0, 64),), -0.2, 0.2), 0.2, 1.0),
        "routes": draw_routes(jax.random.fold_in(streams_of[6], 71), 0),
        "w_gate": bell_draw(streams_of[3], (EXPERTS * GROUP, D, FF_SLICE), D ** -0.5, 0.078125, ((0, 64), (2, 4))),
        "w_up": bell_draw(streams_of[4], (EXPERTS * GROUP, D, FF_SLICE), D ** -0.5, 0.078125, ((0, 64), (2, 4))),
        "w_down": bell_draw(streams_of[5], (EXPERTS * GROUP, FF_SLICE, D), FF ** -0.5, 0.0625, ((0, 64), (1, 4))),
    }


def assignment_slots(routes):
    flat_ids = routes.reshape(-1)
    labels = jnp.arange(EXPERTS, dtype=jnp.int32)
    marked = (flat_ids[:, None] == labels[None, :]).astype(jnp.int32)
    earlier = jnp.cumsum(marked, axis=0) - marked
    return flat_ids, jnp.sum(earlier * marked, axis=1).astype(jnp.int32)


def reference(tokens, mix_weights, routes, w_gate, w_up, w_down):
    flat_ids, slot_ids = assignment_slots(routes)
    token_ids = (jnp.arange(TOKENS * TOP, dtype=jnp.int32) // TOP).astype(jnp.int32)
    slot_grid = slot_ids.reshape(TOKENS, TOP)
    mixed_out = jnp.zeros((TOKENS, D), jnp.float32)
    for expert in range(EXPERTS):
        chosen = (flat_ids == expert) & (slot_ids < CAP)
        target = jnp.where(chosen, slot_ids, CAP).astype(jnp.int32)
        holder = jnp.zeros((CAP + 1,), jnp.int32).at[target].set(token_ids)[:CAP]
        filled = jnp.zeros((CAP + 1,), jnp.int32).at[target].set(1)[:CAP]
        slot_rows = jnp.where(filled[:, None] > 0, tokens[holder], jnp.zeros((), tokens.dtype))
        expert_out = jnp.zeros((CAP, D), jnp.float32)
        for member in range(GROUP):
            weight_row = expert * GROUP + member
            gate_act = jnp.dot(slot_rows, w_gate[weight_row], preferred_element_type=jnp.float32)
            up_act = jnp.dot(slot_rows, w_up[weight_row], preferred_element_type=jnp.float32)
            hidden = (jax.nn.silu(gate_act) * up_act).astype(jnp.bfloat16)
            part_sum = jnp.dot(hidden, w_down[weight_row], preferred_element_type=jnp.float32).astype(jnp.bfloat16)
            expert_out = expert_out + part_sum.astype(jnp.float32)
        for column in range(TOP):
            is_taken = (routes[:, column] == expert) & (slot_grid[:, column] < CAP)
            weight = jnp.where(is_taken, mix_weights[:, column], jnp.zeros((), jnp.float32))
            picked = jnp.take(expert_out, jnp.minimum(slot_grid[:, column], CAP - 1).astype(jnp.int32), axis=0)
            mixed_out = mixed_out + weight[:, None] * picked
    return mixed_out.astype(jnp.bfloat16)
```

```python
import jax
import jax.numpy as jnp
from jax import lax
from jax.sharding import Mesh
from jax.sharding import PartitionSpec as P

EXPERTS = 8
TOP = 2
EXPERT = ("x", "z", "c")
SWAP = [(0, 1), (1, 0)]
BF = jnp.bfloat16
F32 = jnp.float32


def swap_cores(value):
    return lax.ppermute(value, "c", SWAP)


def gather_along(value, axis):
    size = lax.axis_size(axis)
    return lax.all_to_all(
        jnp.broadcast_to(value[None], (size, *value.shape)), axis, 0, 0, tiled=True
    )


def to_lanes(value):
    n, r, f = value.shape
    return jnp.swapaxes(value.reshape(n, r, f // 128, 128), 1, 2).reshape(n, f // 128 * r, 128)


def local(tokens, mix_weights, routes, w_gate, w_up, w_down):
    tok_rows, width = tokens.shape
    xs, zs, ys = lax.axis_size("x"), lax.axis_size("z"), lax.axis_size("y")
    chips = xs * zs
    holders = chips // EXPERTS
    half = width // 2
    most = tok_rows // 2
    rows = 2 * most
    capacity = 5 * tok_rows * chips * 2 * TOP // (4 * EXPERTS)
    core = lax.axis_index("c")

    labels = jnp.arange(EXPERTS, dtype=jnp.int32)
    flat_ids = routes.reshape(-1)
    marked = (flat_ids[:, None] == labels[None, :]).astype(jnp.int32)
    earlier = jnp.cumsum(marked, axis=0) - marked
    rank = jnp.sum(earlier * marked, axis=1)
    counts = jnp.sum(marked, axis=0)
    place = flat_ids * rows + core * most + rank
    hit = (place[:, None] == jnp.arange(EXPERTS * rows, dtype=jnp.int32)[None, :]).reshape(
        tok_rows, TOP, EXPERTS * rows
    )
    pick = jnp.any(hit, axis=1).astype(BF)
    combine = jnp.sum(jnp.where(hit, mix_weights[:, :, None], jnp.zeros((), F32)), axis=1)
    combine_peer = swap_cores(combine)

    packed = jnp.einsum("tp,tf->pf", pick, tokens, preferred_element_type=F32).astype(BF)
    packed = packed.reshape(EXPERTS, rows, width)
    meta = jnp.where(
        jnp.arange(8, dtype=jnp.int32)[None, :, None] == core, counts[:, None, None], 0
    ).astype(BF)
    meta = jnp.broadcast_to(meta, (EXPERTS, 8, 128))
    mine = lax.dynamic_slice_in_dim(packed, core * half, half, axis=2)
    peers = lax.dynamic_slice_in_dim(packed, (1 - core) * half, half, axis=2)
    mine = jnp.concatenate([to_lanes(mine), meta], axis=1)
    peers = jnp.concatenate([to_lanes(peers), meta], axis=1)
    block = mine + swap_cores(peers)
    spread = jnp.broadcast_to(block[:, None], (EXPERTS, holders, *block.shape[1:]))
    arrived = lax.all_to_all(
        spread.reshape(chips, *block.shape[1:]), ("x", "z"), 0, 0, tiled=True
    )

    data_rows = rows * half // 128
    arrived_counts = arrived[:, data_rows : data_rows + 2, 0].astype(jnp.int32).reshape(-1)
    starts = jnp.cumsum(arrived_counts) - arrived_counts
    within = jnp.arange(most, dtype=jnp.int32)
    slot_of = jnp.where(
        within[None, :] < arrived_counts[:, None], starts[:, None] + within[None, :], -1
    ).reshape(-1)
    one_hot = (jnp.arange(capacity, dtype=jnp.int32)[:, None] == slot_of[None, :]).astype(BF)
    data = arrived[:, :data_rows].reshape(chips, half // 128, rows, 128)
    data = jnp.swapaxes(data, 1, 2).reshape(chips * rows, half)
    in_rows = jnp.dot(one_hot, data, preferred_element_type=F32).astype(BF)

    own = gather_along(in_rows, "y")
    other = swap_cores(own)
    gate_w = w_gate[0].reshape(ys, 2, half, -1)
    up_w = w_up[0].reshape(ys, 2, half, -1)
    down_w = w_down[0].reshape(-1, ys, 2, half)
    gate_act = jnp.zeros((), F32)
    up_act = jnp.zeros((), F32)
    for part, at in ((own, core), (other, 1 - core)):
        gw = lax.dynamic_index_in_dim(gate_w, at, 1, keepdims=False)
        uw = lax.dynamic_index_in_dim(up_w, at, 1, keepdims=False)
        for y in range(ys):
            gate_act = gate_act + jnp.dot(part[y], gw[y], preferred_element_type=F32)
            up_act = up_act + jnp.dot(part[y], uw[y], preferred_element_type=F32)
    hidden = (jax.nn.silu(gate_act) * up_act).astype(BF)

    def down(at):
        dw = lax.dynamic_index_in_dim(down_w, at, 2, keepdims=False)
        return jnp.stack(
            [jnp.dot(hidden, dw[:, y], preferred_element_type=F32) for y in range(ys)]
        )

    from_peer = swap_cores(down(1 - core).astype(BF))
    chip_sum = (down(core) + from_peer.astype(F32)).astype(BF)
    shares = lax.all_to_all(chip_sum, "y", 0, 0, tiled=True)
    reduced = jnp.sum(shares.astype(F32), axis=0).astype(BF)

    back = lax.dot_general(
        one_hot, reduced, (((0,), (0,)), ((), ())), preferred_element_type=F32
    ).astype(BF)
    returned = lax.all_to_all(back.reshape(chips, rows, half), ("x", "z"), 0, 0, tiled=True)
    summed = jnp.sum(
        returned.reshape(EXPERTS, holders, rows, half).astype(F32), axis=1
    ).reshape(EXPERTS * rows, half)
    out_own = jnp.dot(combine, summed, precision=lax.Precision.HIGHEST).astype(BF)
    out_peer = jnp.dot(combine_peer, summed, precision=lax.Precision.HIGHEST).astype(BF)
    out_swap = swap_cores(out_peer)
    low = jnp.where(core == 0, out_own, out_swap)
    high = jnp.where(core == 0, out_swap, out_own)
    return jnp.concatenate([low, high], axis=1)


def solution(mesh):
    chips = Mesh(mesh.devices.reshape(4, 8, 2, mesh.shape["mp"]), ("x", "z", "c", "y"))
    placed = (
        P(EXPERT, "y"),
        P(EXPERT, None),
        P(EXPERT, None),
        P(EXPERT, None, "y"),
        P(EXPERT, None, "y"),
        P(EXPERT, "y", None),
    )
    return jax.shard_map(
        local, mesh=chips, in_specs=placed, out_specs=P(EXPERT, "y"), check_vma=False
    )
```

```python
import math

import jax
import jax.numpy as jnp
from jax import lax
from jax.experimental import pallas as pl
from jax.experimental.pallas import tpu as pltpu
from jax.sharding import Mesh
from jax.sharding import PartitionSpec as P


EXPERTS = 8
TOP = 2
EXPERT = ("x", "z", "c")
SWAP = [(0, 1), (1, 0)]
BF = jnp.bfloat16
F32 = jnp.float32


def swap_cores(value):
    return lax.ppermute(value, "c", SWAP)


def shift(value, axis, by):
    size = lax.axis_size(axis)
    return lax.ppermute(value, axis, [(i, (i + by) % size) for i in range(size)])


def shift_y(value, by):
    return shift(value, "y", by)


def to_lanes(value):
    n, r, f = value.shape
    return jnp.swapaxes(value.reshape(n, r, f // 128, 128), 1, 2).reshape(n, f // 128 * r, 128)


VMEM = pl.BlockSpec(memory_space=pltpu.VMEM)


def near(value):
    return pltpu.with_memory_space_constraint(value, pltpu.VMEM)


def column(at):
    off, peer = at
    size = lax.axis_size("y")
    core = lax.axis_index("c")
    return (lax.axis_index("y") + off + size) % size * 2 + (1 - core if peer else core)


def cost(flops, *shapes):
    moved = sum(math.prod(shape) * 2 for shape in shapes)
    return pl.CostEstimate(flops=flops, transcendentals=0, bytes_accessed=moved)


def gate_up_body(pieces, ats, first, sends, *refs):
    xs = refs[: len(pieces)]
    gate_w, up_w = refs[len(pieces) : len(pieces) + 2]
    refs = refs[len(pieces) + 2 :]
    if not first:
        gate_in, up_in = refs[:2]
        refs = refs[2:]
    if sends:
        down_w = refs[0]
        outs = refs[1 : 1 + len(sends)]
        gate_acc, up_acc = refs[1 + len(sends) :]
    else:
        gate_acc, up_acc = refs
    block = xs[0].shape[1]
    done = set()
    for x_ref, (j, low, high) in zip(xs, pieces):
        rows = pl.ds(pl.multiple_of(column(ats[j]) * block, block), block)
        x = x_ref[...]
        g = jnp.dot(x, gate_w[rows, :], preferred_element_type=F32)
        u = jnp.dot(x, up_w[rows, :], preferred_element_type=F32)
        if low in done:
            gate_acc[low:high, :] += g
            up_acc[low:high, :] += u
        elif first:
            gate_acc[low:high, :] = g
            up_acc[low:high, :] = u
        else:
            gate_acc[low:high, :] = gate_in[low:high, :] + g
            up_acc[low:high, :] = up_in[low:high, :] + u
        done.add(low)
    if not sends:
        return
    gate = gate_acc[...]
    hidden = (gate / (1.0 + jnp.exp(-gate)) * up_acc[...]).astype(BF)
    for j, at in enumerate(sends):
        cols = pl.ds(pl.multiple_of(column(at) * block, 128), block)
        outs[j][...] = jnp.dot(hidden, down_w[:, cols], preferred_element_type=F32).astype(BF)


def gate_up(xs, pieces, ats, gate_rows, up_rows, carried, rows, down_rows=None, sends=()):
    block = xs[0].shape[1]
    units = gate_rows.shape[1]
    first = carried is None
    if sends:
        out = [pltpu.VMEM((rows, block), BF)] * len(sends)
    else:
        out = [pltpu.VMEM((rows, units), F32)] * 2
    n = len(ats)

    def body(*refs):
        gate_up_body(pieces, ats, first, sends, *refs)

    inputs = [*xs, gate_rows, up_rows]
    inputs += [] if first else carried
    inputs += [down_rows] if sends else []
    return pl.pallas_call(
        body,
        out_shape=out,
        in_specs=[VMEM] * len(inputs),
        out_specs=[VMEM] * len(out),
        scratch_shapes=[pltpu.VMEM((rows, units), F32)] * 2 if sends else [],
        compiler_params=pltpu.CompilerParams(vmem_limit_bytes=16 * 2**20),
        cost_estimate=cost(
            2 * rows * block * units * (2 * n + len(sends)),
            (2 * n + len(sends), block, units), (n + len(sends), rows, block), (8, rows, units),
        ),
        name="gate_up_down" if sends else "gate_up",
    )(*[near(v) for v in inputs])


def layer(tokens, mix_weights, routes, w_gate, w_up, w_down):
    tok_rows, width = tokens.shape
    xs, zs = lax.axis_size("x"), lax.axis_size("z")
    chips = xs * zs
    holders = chips // EXPERTS
    half = width // 2
    most = tok_rows // 2
    rows = 2 * most
    capacity = 5 * tok_rows * chips * 2 * TOP // (4 * EXPERTS)
    core = lax.axis_index("c")

    labels = jnp.arange(EXPERTS, dtype=jnp.int32)
    flat_ids = routes.reshape(-1)
    marked = (flat_ids[:, None] == labels[None, :]).astype(jnp.int32)
    earlier = jnp.cumsum(marked, axis=0) - marked
    rank = jnp.sum(earlier * marked, axis=1)
    counts = jnp.sum(marked, axis=0)
    place = flat_ids * rows + core * most + rank
    hit = (place[:, None] == jnp.arange(EXPERTS * rows, dtype=jnp.int32)[None, :]).reshape(
        tok_rows, TOP, EXPERTS * rows
    )
    pick = jnp.any(hit, axis=1).astype(BF)
    combine = jnp.sum(jnp.where(hit, mix_weights[:, :, None], jnp.zeros((), F32)), axis=1)

    packed = jnp.einsum("tp,tf->pf", pick, tokens, preferred_element_type=F32).astype(BF)
    packed = packed.reshape(EXPERTS, rows, width)
    meta = jnp.where(
        jnp.arange(8, dtype=jnp.int32)[None, :, None] == core, counts[:, None, None], 0
    ).astype(BF)
    meta = jnp.broadcast_to(meta, (EXPERTS, 8, 128))
    mine = lax.dynamic_slice_in_dim(packed, core * half, half, axis=2)
    peers = lax.dynamic_slice_in_dim(packed, (1 - core) * half, half, axis=2)
    mine = jnp.concatenate([meta, to_lanes(mine)], axis=1)
    peers = jnp.concatenate([meta, to_lanes(peers)], axis=1)
    blocks = mine + swap_cores(peers)
    combine_peer = swap_cores(combine)
    spread = jnp.broadcast_to(blocks[:, None], (EXPERTS, holders, *blocks.shape[1:]))
    arrived = lax.all_to_all(
        spread.reshape(chips, *blocks.shape[1:]), ("x", "z"), 0, 0, tiled=True
    )

    arrived_counts = arrived[:, 0:2, 0].astype(jnp.int32).reshape(-1)
    starts = jnp.cumsum(arrived_counts) - arrived_counts
    within = jnp.arange(most, dtype=jnp.int32)
    slot_of = jnp.where(
        within[None, :] < arrived_counts[:, None], starts[:, None] + within[None, :], -1
    ).reshape(-1)
    one_hot = (jnp.arange(capacity, dtype=jnp.int32)[:, None] == slot_of[None, :]).astype(BF)
    data = jnp.swapaxes(arrived[:, 8:].reshape(chips, half // 128, rows, 128), 1, 2)
    data = data.reshape(chips * rows, half)

    mid = capacity // 2
    gate_rows, up_rows, down_rows = w_gate[0], w_up[0], w_down[0]
    top = jnp.dot(one_hot[:mid], data, preferred_element_type=F32).astype(BF)
    bottom = jnp.dot(one_hot[mid:], data, preferred_element_type=F32).astype(BF)
    below_top = shift_y(top, 1)
    above_bottom = shift_y(bottom, -1)
    below_bottom = shift_y(bottom, 1)
    above_top = shift_y(top, -1)
    far_top = shift_y(below_top, 1)
    far_bottom = shift_y(above_bottom, -1)
    acts = gate_up(
        [top, bottom, swap_cores(top), swap_cores(bottom)],
        [(0, 0, mid), (0, mid, capacity), (1, 0, mid), (1, mid, capacity)],
        ((0, 0), (0, 1)),
        gate_rows, up_rows, None, capacity,
    )
    around = ((-1, 0), (1, 0), (-1, 1), (1, 1))
    for close, top_at, bottom_at in (
        ([below_top, above_bottom], 0, 1), ([above_top, below_bottom], 1, 0)
    ):
        acts = gate_up(
            close + [swap_cores(v) for v in close],
            [
                (top_at, 0, mid),
                (bottom_at, mid, capacity),
                (top_at + 2, 0, mid),
                (bottom_at + 2, mid, capacity),
            ],
            around,
            gate_rows, up_rows, acts, capacity,
        )
    far = [far_top, far_bottom]
    order = (2, 1, -1, 0)
    parts = gate_up(
        far + [swap_cores(v) for v in far],
        [(0, 0, mid), (0, mid, capacity), (1, 0, mid), (1, mid, capacity)],
        ((2, 0), (2, 1)),
        gate_rows, up_rows, acts, capacity,
        down_rows, tuple((off, 1) for off in order) + tuple((off, 0) for off in order),
    )

    def add(*values):
        return sum(v.astype(F32) for v in values).astype(BF)

    def chip_sums(k, peer):
        return lax.optimization_barrier(
            (add(parts[4 + k][:mid], peer[:mid]), add(parts[4 + k][mid:], peer[mid:]))
        )

    peers = [swap_cores(v) for v in parts[:4]]
    far_top, far_bottom = chip_sums(0, peers[0])
    top_in = shift_y(far_top, 1)
    bottom_in = shift_y(far_bottom, -1)
    up_top, up_bottom = chip_sums(1, peers[1])
    dn_top, dn_bottom = chip_sums(2, peers[2])
    below_bottom = shift_y(up_bottom, 1)
    above_top = shift_y(dn_top, -1)
    below_top = shift_y(lax.optimization_barrier(add(up_top, top_in)), 1)
    above_bottom = shift_y(lax.optimization_barrier(add(dn_bottom, bottom_in)), -1)
    part_own, peer_own = parts[7], peers[3]
    reduced = jnp.concatenate(
        [
            add(part_own[:mid], peer_own[:mid], below_top, above_top),
            add(part_own[mid:], peer_own[mid:], below_bottom, above_bottom),
        ]
    )

    back = lax.dot_general(
        one_hot, reduced, (((0,), (0,)), ((), ())), preferred_element_type=F32
    ).astype(BF)
    returned = lax.all_to_all(back.reshape(chips, rows, half), ("x", "z"), 0, 0, tiled=True)
    summed = jnp.sum(
        returned.reshape(EXPERTS, holders, rows, half).astype(F32), axis=1
    ).reshape(EXPERTS * rows, half)
    out_own = jnp.dot(combine, summed, precision=lax.Precision.HIGHEST).astype(BF)
    out_peer = jnp.dot(combine_peer, summed, precision=lax.Precision.HIGHEST).astype(BF)
    out_swap = swap_cores(out_peer)
    low = jnp.where(core == 0, out_own, out_swap)
    high = jnp.where(core == 0, out_swap, out_own)
    return jnp.concatenate([low, high], axis=1)


def solution(mesh):
    chips = Mesh(mesh.devices.reshape(4, 8, 2, mesh.shape["mp"]), ("x", "z", "c", "y"))
    placed = (
        P(EXPERT, "y"),
        P(EXPERT, None),
        P(EXPERT, None),
        P(EXPERT, None, "y"),
        P(EXPERT, None, "y"),
        P(EXPERT, "y", None),
    )
    return jax.shard_map(
        layer, mesh=chips, in_specs=placed, out_specs=P(EXPERT, "y"), check_vma=False
    )
```

```python
import math

import jax
import jax.numpy as jnp
from jax import lax
from jax.experimental import pallas as pl
from jax.experimental.pallas import tpu as pltpu
from jax.sharding import Mesh
from jax.sharding import PartitionSpec as P


EXPERTS = 8
TOP = 2
EMPTY = 256.0
EXPERT = ("x", "z", "c")
SWAP = [(0, 1), (1, 0)]
BF = jnp.bfloat16
F32 = jnp.float32


def swap_cores(value):
    return lax.ppermute(value, "c", SWAP)


def shift(value, axis, by):
    size = lax.axis_size(axis)
    return lax.ppermute(value, axis, [(i, (i + by) % size) for i in range(size)])


def shift_y(value, by):
    return shift(value, "y", by)


VMEM = pl.BlockSpec(memory_space=pltpu.VMEM)


def near(value):
    return pltpu.with_memory_space_constraint(value, pltpu.VMEM)


def column(at):
    off, peer = at
    size = lax.axis_size("y")
    core = lax.axis_index("c")
    return (lax.axis_index("y") + off + size) % size * 2 + (1 - core if peer else core)


def cost(flops, *shapes):
    moved = sum(math.prod(shape) * 2 for shape in shapes)
    return pl.CostEstimate(flops=flops, transcendentals=0, bytes_accessed=moved)


def pack_body(routes_ref, tokens_ref, mine_ref, peers_ref, stage):
    tok_rows, width = tokens_ref.shape
    rows = tok_rows
    most = tok_rows // 2
    half = width // 2
    slots = EXPERTS * rows
    core = lax.axis_index("c")

    def iota(shape, dim):
        return lax.broadcasted_iota(jnp.int32, shape, dim)

    experts = iota((tok_rows, EXPERTS), 1)
    hits = (routes_ref[:, 0:1] == experts) | (routes_ref[:, 1:2] == experts)
    hits = hits.astype(F32)
    before = (iota((tok_rows, tok_rows), 1) < iota((tok_rows, tok_rows), 0)).astype(F32)
    rank = jnp.dot(before, hits, preferred_element_type=F32)
    counts = jnp.dot(jnp.ones((8, tok_rows), F32), hits, preferred_element_type=F32)
    lane = iota((EXPERTS, slots), 1)
    low = iota((EXPERTS, slots), 0) * rows
    expand = ((lane >= low) & (lane < low + rows)).astype(F32)

    def place(n):
        at = iota((n, slots), 1)
        first = sum((at >= e * rows).astype(jnp.int32) for e in range(1, EXPERTS)) * rows
        return at - first - core * most

    hit = jnp.dot(hits, expand, preferred_element_type=F32) > 0.5
    rank = jnp.dot(rank, expand, preferred_element_type=F32).astype(jnp.int32)
    counts = jnp.dot(counts, expand, preferred_element_type=F32).astype(jnp.int32)
    pick = jnp.where(hit & (rank == place(tok_rows)), 1.0, 0.0).astype(BF)
    empty = (place(8) >= counts) & (place(8) < most) & (iota((8, slots), 0) == 0)
    empty = jnp.where(empty, 1.0, 0.0).astype(BF)
    over_rows = (((0,), (0,)), ((), ()))
    stage[...] = lax.dot_general(
        pick, tokens_ref[...], over_rows, preferred_element_type=F32
    ) + lax.dot_general(
        empty, jnp.full((8, width), EMPTY, BF), over_rows, preferred_element_type=F32
    )
    for e in range(EXPERTS):
        for f in range(half // 128):
            for out, side in ((mine_ref, core), (peers_ref, 1 - core)):
                lanes = pl.ds(pl.multiple_of(side * half + f * 128, 128), 128)
                out[e, f * rows : (f + 1) * rows, :] = stage[
                    e * rows : (e + 1) * rows, lanes
                ].astype(BF)


def pack(routes, tokens):
    tok_rows, width = tokens.shape
    out = pltpu.VMEM((EXPERTS, width // 256 * tok_rows, 128), BF)
    return pl.pallas_call(
        pack_body,
        out_shape=[out, out],
        in_specs=[VMEM] * 2,
        out_specs=[VMEM] * 2,
        scratch_shapes=[pltpu.VMEM((EXPERTS * tok_rows, width), F32)],
        compiler_params=pltpu.CompilerParams(vmem_limit_bytes=16 * 2**20),
        name="pack",
    )(near(routes), near(tokens))


def gate_up_body(pieces, ats, first, sends, *refs):
    xs = refs[: len(pieces)]
    gate_w, up_w = refs[len(pieces) : len(pieces) + 2]
    refs = refs[len(pieces) + 2 :]
    if not first:
        gate_in, up_in = refs[:2]
        refs = refs[2:]
    if sends:
        down_w = refs[0]
        outs = refs[1 : 1 + len(sends)]
        gate_acc, up_acc = refs[1 + len(sends) :]
    else:
        gate_acc, up_acc = refs
    block = xs[0].shape[1]
    done = set()
    for x_ref, (j, low, high) in zip(xs, pieces):
        rows = pl.ds(pl.multiple_of(column(ats[j]) * block, block), block)
        x = x_ref[...]
        g = jnp.dot(x, gate_w[rows, :], preferred_element_type=F32)
        u = jnp.dot(x, up_w[rows, :], preferred_element_type=F32)
        if low in done:
            gate_acc[low:high, :] += g
            up_acc[low:high, :] += u
        elif first:
            gate_acc[low:high, :] = g
            up_acc[low:high, :] = u
        else:
            gate_acc[low:high, :] = gate_in[low:high, :] + g
            up_acc[low:high, :] = up_in[low:high, :] + u
        done.add(low)
    if not sends:
        return
    gate = gate_acc[...]
    hidden = (gate / (1.0 + jnp.exp(-gate)) * up_acc[...]).astype(BF)
    for j, at in enumerate(sends):
        cols = pl.ds(pl.multiple_of(column(at) * block, 128), block)
        outs[j][...] = jnp.dot(hidden, down_w[:, cols], preferred_element_type=F32).astype(BF)


def gate_up(xs, pieces, ats, gate_rows, up_rows, carried, rows, down_rows=None, sends=()):
    block = xs[0].shape[1]
    units = gate_rows.shape[1]
    first = carried is None
    if sends:
        out = [pltpu.VMEM((rows, block), BF)] * len(sends)
    else:
        out = [pltpu.VMEM((rows, units), F32)] * 2
    n = len(ats)

    def body(*refs):
        gate_up_body(pieces, ats, first, sends, *refs)

    inputs = [*xs, gate_rows, up_rows]
    inputs += [] if first else carried
    inputs += [down_rows] if sends else []
    return pl.pallas_call(
        body,
        out_shape=out,
        in_specs=[VMEM] * len(inputs),
        out_specs=[VMEM] * len(out),
        scratch_shapes=[pltpu.VMEM((rows, units), F32)] * 2 if sends else [],
        compiler_params=pltpu.CompilerParams(vmem_limit_bytes=16 * 2**20),
        cost_estimate=cost(
            2 * rows * block * units * (2 * n + len(sends)),
            (2 * n + len(sends), block, units), (n + len(sends), rows, block), (8, rows, units),
        ),
        name="gate_up_down" if sends else "gate_up",
    )(*[near(v) for v in inputs])


def layer(tokens, mix_weights, routes, w_gate, w_up, w_down):
    tok_rows, width = tokens.shape
    xs, zs = lax.axis_size("x"), lax.axis_size("z")
    chips = xs * zs
    holders = chips // EXPERTS
    half = width // 2
    most = tok_rows // 2
    rows = 2 * most
    capacity = 5 * tok_rows * chips * 2 * TOP // (4 * EXPERTS)
    core = lax.axis_index("c")

    labels = jnp.arange(EXPERTS, dtype=jnp.int32)
    flat_ids = routes.reshape(-1)
    marked = (flat_ids[:, None] == labels[None, :]).astype(jnp.int32)
    earlier = jnp.cumsum(marked, axis=0) - marked
    rank = jnp.sum(earlier * marked, axis=1)
    place = flat_ids * rows + core * most + rank
    hit = (place[:, None] == jnp.arange(EXPERTS * rows, dtype=jnp.int32)[None, :]).reshape(
        tok_rows, TOP, EXPERTS * rows
    )
    pick = jnp.any(hit, axis=1).astype(BF)
    combine = jnp.sum(jnp.where(hit, mix_weights[:, :, None], jnp.zeros((), F32)), axis=1)

    mine, peers = pack(routes, tokens)
    blocks = mine + swap_cores(peers)
    combine_peer = swap_cores(combine)
    spread = jnp.broadcast_to(blocks[:, None], (EXPERTS, holders, *blocks.shape[1:]))
    arrived = lax.all_to_all(
        spread.reshape(chips, *blocks.shape[1:]), ("x", "z"), 0, 0, tiled=True
    )

    filled = (arrived[:, :rows, 0].astype(F32) < EMPTY / 2).astype(jnp.int32)
    arrived_counts = jnp.sum(filled.reshape(chips * 2, most), axis=1)
    starts = jnp.cumsum(arrived_counts) - arrived_counts
    within = jnp.arange(most, dtype=jnp.int32)
    slot_of = jnp.where(
        within[None, :] < arrived_counts[:, None], starts[:, None] + within[None, :], -1
    ).reshape(-1)
    one_hot = (jnp.arange(capacity, dtype=jnp.int32)[:, None] == slot_of[None, :]).astype(BF)
    data = jnp.swapaxes(arrived.reshape(chips, half // 128, rows, 128), 1, 2)
    data = data.reshape(chips * rows, half)

    mid = capacity // 2
    gate_rows, up_rows, down_rows = w_gate[0], w_up[0], w_down[0]
    top = jnp.dot(one_hot[:mid], data, preferred_element_type=F32).astype(BF)
    bottom = jnp.dot(one_hot[mid:], data, preferred_element_type=F32).astype(BF)
    below_top = shift_y(top, 1)
    above_bottom = shift_y(bottom, -1)
    below_bottom = shift_y(bottom, 1)
    above_top = shift_y(top, -1)
    far_top = shift_y(below_top, 1)
    far_bottom = shift_y(above_bottom, -1)
    acts = gate_up(
        [top, bottom, swap_cores(top), swap_cores(bottom)],
        [(0, 0, mid), (0, mid, capacity), (1, 0, mid), (1, mid, capacity)],
        ((0, 0), (0, 1)),
        gate_rows, up_rows, None, capacity,
    )
    around = ((-1, 0), (1, 0), (-1, 1), (1, 1))
    for close, top_at, bottom_at in (
        ([below_top, above_bottom], 0, 1), ([above_top, below_bottom], 1, 0)
    ):
        acts = gate_up(
            close + [swap_cores(v) for v in close],
            [
                (top_at, 0, mid),
                (bottom_at, mid, capacity),
                (top_at + 2, 0, mid),
                (bottom_at + 2, mid, capacity),
            ],
            around,
            gate_rows, up_rows, acts, capacity,
        )
    far = [far_top, far_bottom]
    order = (2, 1, -1, 0)
    parts = gate_up(
        far + [swap_cores(v) for v in far],
        [(0, 0, mid), (0, mid, capacity), (1, 0, mid), (1, mid, capacity)],
        ((2, 0), (2, 1)),
        gate_rows, up_rows, acts, capacity,
        down_rows, tuple((off, 1) for off in order) + tuple((off, 0) for off in order),
    )

    def add(*values):
        return sum(v.astype(F32) for v in values).astype(BF)

    def chip_sums(k, peer):
        return lax.optimization_barrier(
            (add(parts[4 + k][:mid], peer[:mid]), add(parts[4 + k][mid:], peer[mid:]))
        )

    peers = [swap_cores(v) for v in parts[:4]]
    far_top, far_bottom = chip_sums(0, peers[0])
    top_in = shift_y(far_top, 1)
    bottom_in = shift_y(far_bottom, -1)
    up_top, up_bottom = chip_sums(1, peers[1])
    dn_top, dn_bottom = chip_sums(2, peers[2])
    below_bottom = shift_y(up_bottom, 1)
    above_top = shift_y(dn_top, -1)
    below_top = shift_y(lax.optimization_barrier(add(up_top, top_in)), 1)
    above_bottom = shift_y(lax.optimization_barrier(add(dn_bottom, bottom_in)), -1)
    part_own, peer_own = parts[7], peers[3]
    reduced = jnp.concatenate(
        [
            add(part_own[:mid], peer_own[:mid], below_top, above_top),
            add(part_own[mid:], peer_own[mid:], below_bottom, above_bottom),
        ]
    )

    back = lax.dot_general(
        one_hot, reduced, (((0,), (0,)), ((), ())), preferred_element_type=F32
    ).astype(BF)
    returned = lax.all_to_all(back.reshape(chips, rows, half), ("x", "z"), 0, 0, tiled=True)
    summed = jnp.sum(
        returned.reshape(EXPERTS, holders, rows, half).astype(F32), axis=1
    ).reshape(EXPERTS * rows, half)
    out_own = jnp.dot(combine, summed, precision=lax.Precision.HIGHEST).astype(BF)
    out_peer = jnp.dot(combine_peer, summed, precision=lax.Precision.HIGHEST).astype(BF)
    out_swap = swap_cores(out_peer)
    low = jnp.where(core == 0, out_own, out_swap)
    high = jnp.where(core == 0, out_swap, out_own)
    return jnp.concatenate([low, high], axis=1)


def solution(mesh):
    chips = Mesh(mesh.devices.reshape(4, 8, 2, mesh.shape["mp"]), ("x", "z", "c", "y"))
    placed = (
        P(EXPERT, "y"),
        P(EXPERT, None),
        P(EXPERT, None),
        P(EXPERT, None, "y"),
        P(EXPERT, None, "y"),
        P(EXPERT, "y", None),
    )
    return jax.shard_map(
        layer, mesh=chips, in_specs=placed, out_specs=P(EXPERT, "y"), check_vma=False
    )
```

```python
import math

import jax
import jax.numpy as jnp
from jax import lax
from jax.experimental import pallas as pl
from jax.experimental.pallas import tpu as pltpu
from jax.sharding import Mesh
from jax.sharding import PartitionSpec as P


EXPERTS = 8
TOP = 2
EMPTY = 256.0
EXPERT = ("x", "z", "c")
SWAP = [(0, 1), (1, 0)]
BF = jnp.bfloat16
F32 = jnp.float32


def swap_cores(value):
    return lax.ppermute(value, "c", SWAP)


def shift(value, axis, by):
    size = lax.axis_size(axis)
    return lax.ppermute(value, axis, [(i, (i + by) % size) for i in range(size)])


def shift_y(value, by):
    return shift(value, "y", by)


VMEM = pl.BlockSpec(memory_space=pltpu.VMEM)


def near(value):
    return pltpu.with_memory_space_constraint(value, pltpu.VMEM)


def column(at):
    off, peer = at
    size = lax.axis_size("y")
    core = lax.axis_index("c")
    return (lax.axis_index("y") + off + size) % size * 2 + (1 - core if peer else core)


def cost(flops, *shapes):
    moved = sum(math.prod(shape) * 2 for shape in shapes)
    return pl.CostEstimate(flops=flops, transcendentals=0, bytes_accessed=moved)


def pack_body(routes_ref, tokens_ref, mine_ref, peers_ref, stage):
    tok_rows, width = tokens_ref.shape
    rows = tok_rows
    most = tok_rows // 2
    half = width // 2
    slots = EXPERTS * rows
    core = lax.axis_index("c")

    def iota(shape, dim):
        return lax.broadcasted_iota(jnp.int32, shape, dim)

    experts = iota((tok_rows, EXPERTS), 1)
    hits = (routes_ref[:, 0:1] == experts) | (routes_ref[:, 1:2] == experts)
    hits = hits.astype(F32)
    before = (iota((tok_rows, tok_rows), 1) < iota((tok_rows, tok_rows), 0)).astype(F32)
    rank = jnp.dot(before, hits, preferred_element_type=F32)
    counts = jnp.dot(jnp.ones((8, tok_rows), F32), hits, preferred_element_type=F32)
    lane = iota((EXPERTS, slots), 1)
    low = iota((EXPERTS, slots), 0) * rows
    expand = ((lane >= low) & (lane < low + rows)).astype(F32)

    def place(n):
        at = iota((n, slots), 1)
        first = sum((at >= e * rows).astype(jnp.int32) for e in range(1, EXPERTS)) * rows
        return at - first - core * most

    hit = jnp.dot(hits, expand, preferred_element_type=F32) > 0.5
    rank = jnp.dot(rank, expand, preferred_element_type=F32).astype(jnp.int32)
    counts = jnp.dot(counts, expand, preferred_element_type=F32).astype(jnp.int32)
    pick = jnp.where(hit & (rank == place(tok_rows)), 1.0, 0.0).astype(BF)
    empty = (place(8) >= counts) & (place(8) < most) & (iota((8, slots), 0) == 0)
    empty = jnp.where(empty, 1.0, 0.0).astype(BF)
    over_rows = (((0,), (0,)), ((), ()))
    stage[...] = lax.dot_general(
        pick, tokens_ref[...], over_rows, preferred_element_type=F32
    ) + lax.dot_general(
        empty, jnp.full((8, width), EMPTY, BF), over_rows, preferred_element_type=F32
    )
    for e in range(EXPERTS):
        for f in range(half // 128):
            for out, side in ((mine_ref, core), (peers_ref, 1 - core)):
                lanes = pl.ds(pl.multiple_of(side * half + f * 128, 128), 128)
                out[e, f * rows : (f + 1) * rows, :] = stage[
                    e * rows : (e + 1) * rows, lanes
                ].astype(BF)


def pack(routes, tokens):
    tok_rows, width = tokens.shape
    out = pltpu.VMEM((EXPERTS, width // 256 * tok_rows, 128), BF)
    return pl.pallas_call(
        pack_body,
        out_shape=[out, out],
        in_specs=[VMEM] * 2,
        out_specs=[VMEM] * 2,
        scratch_shapes=[pltpu.VMEM((EXPERTS * tok_rows, width), F32)],
        compiler_params=pltpu.CompilerParams(vmem_limit_bytes=16 * 2**20),
        name="pack",
    )(near(routes), near(tokens))


def gate_up_body(pieces, ats, first, sends, *refs):
    xs = refs[: len(pieces)]
    gate_w, up_w = refs[len(pieces) : len(pieces) + 2]
    refs = refs[len(pieces) + 2 :]
    if not first:
        gate_in, up_in = refs[:2]
        refs = refs[2:]
    if sends:
        down_w, hidden_ref = refs[:2]
        outs = refs[2 : 2 + len(sends)]
        gate_acc, up_acc = refs[2 + len(sends) :]
    else:
        gate_acc, up_acc = refs
    block = xs[0].shape[1]
    done = set()
    for x_ref, (j, low, high) in zip(xs, pieces):
        rows = pl.ds(pl.multiple_of(column(ats[j]) * block, block), block)
        x = x_ref[...]
        g = jnp.dot(x, gate_w[rows, :], preferred_element_type=F32)
        u = jnp.dot(x, up_w[rows, :], preferred_element_type=F32)
        if low in done:
            gate_acc[low:high, :] += g
            up_acc[low:high, :] += u
        elif first:
            gate_acc[low:high, :] = g
            up_acc[low:high, :] = u
        else:
            gate_acc[low:high, :] = gate_in[low:high, :] + g
            up_acc[low:high, :] = up_in[low:high, :] + u
        done.add(low)
    if not sends:
        return
    gate = gate_acc[...]
    hidden = (gate / (1.0 + jnp.exp(-gate)) * up_acc[...]).astype(BF)
    hidden_ref[...] = hidden
    project(hidden, down_w, sends, outs)


def project(hidden, down_w, sends, outs):
    block = outs[0].shape[1]
    for j, at in enumerate(sends):
        cols = pl.ds(pl.multiple_of(column(at) * block, 128), block)
        outs[j][...] = jnp.dot(hidden, down_w[:, cols], preferred_element_type=F32).astype(BF)


def down(hidden, down_rows, sends, block):
    def body(hidden_ref, down_w, *outs):
        project(hidden_ref[...], down_w, sends, outs)

    rows, units = hidden.shape
    n = len(sends)
    return pl.pallas_call(
        body,
        out_shape=[pltpu.VMEM((rows, block), BF)] * n,
        in_specs=[VMEM] * 2,
        out_specs=[VMEM] * n,
        compiler_params=pltpu.CompilerParams(vmem_limit_bytes=16 * 2**20),
        cost_estimate=cost(2 * n * rows * units * block, (n, units, block), (n, rows, block)),
        name="down",
    )(near(hidden), near(down_rows))


def gate_up(xs, pieces, ats, gate_rows, up_rows, carried, rows, down_rows=None, sends=()):
    block = xs[0].shape[1]
    units = gate_rows.shape[1]
    first = carried is None
    if sends:
        out = [pltpu.VMEM((rows, units), BF)]
        out += [pltpu.VMEM((rows, block), BF)] * len(sends)
    else:
        out = [pltpu.VMEM((rows, units), F32)] * 2
    n = len(ats)

    def body(*refs):
        gate_up_body(pieces, ats, first, sends, *refs)

    inputs = [*xs, gate_rows, up_rows]
    inputs += [] if first else carried
    inputs += [down_rows] if sends else []
    return pl.pallas_call(
        body,
        out_shape=out,
        in_specs=[VMEM] * len(inputs),
        out_specs=[VMEM] * len(out),
        scratch_shapes=[pltpu.VMEM((rows, units), F32)] * 2 if sends else [],
        compiler_params=pltpu.CompilerParams(vmem_limit_bytes=16 * 2**20),
        cost_estimate=cost(
            2 * rows * block * units * (2 * n + len(sends)),
            (2 * n + len(sends), block, units), (n + len(sends), rows, block), (8, rows, units),
        ),
        name="gate_up_down" if sends else "gate_up",
    )(*[near(v) for v in inputs])


def layer(tokens, mix_weights, routes, w_gate, w_up, w_down):
    tok_rows, width = tokens.shape
    xs, zs = lax.axis_size("x"), lax.axis_size("z")
    chips = xs * zs
    holders = chips // EXPERTS
    half = width // 2
    most = tok_rows // 2
    rows = 2 * most
    capacity = 5 * tok_rows * chips * 2 * TOP // (4 * EXPERTS)
    core = lax.axis_index("c")

    labels = jnp.arange(EXPERTS, dtype=jnp.int32)
    flat_ids = routes.reshape(-1)
    marked = (flat_ids[:, None] == labels[None, :]).astype(jnp.int32)
    earlier = jnp.cumsum(marked, axis=0) - marked
    rank = jnp.sum(earlier * marked, axis=1)
    place = flat_ids * rows + core * most + rank
    hit = (place[:, None] == jnp.arange(EXPERTS * rows, dtype=jnp.int32)[None, :]).reshape(
        tok_rows, TOP, EXPERTS * rows
    )
    pick = jnp.any(hit, axis=1).astype(BF)
    combine = jnp.sum(jnp.where(hit, mix_weights[:, :, None], jnp.zeros((), F32)), axis=1)

    mine, peers = pack(routes, tokens)
    blocks = mine + swap_cores(peers)
    combine_peer = swap_cores(combine)
    spread = jnp.broadcast_to(blocks[:, None], (EXPERTS, holders, *blocks.shape[1:]))
    arrived = lax.all_to_all(
        spread.reshape(chips, *blocks.shape[1:]), ("x", "z"), 0, 0, tiled=True
    )

    filled = (arrived[:, :rows, 0].astype(F32) < EMPTY / 2).astype(jnp.int32)
    arrived_counts = jnp.sum(filled.reshape(chips * 2, most), axis=1)
    starts = jnp.cumsum(arrived_counts) - arrived_counts
    within = jnp.arange(most, dtype=jnp.int32)
    slot_of = jnp.where(
        within[None, :] < arrived_counts[:, None], starts[:, None] + within[None, :], -1
    ).reshape(-1)
    one_hot = (jnp.arange(capacity, dtype=jnp.int32)[:, None] == slot_of[None, :]).astype(BF)
    data = jnp.swapaxes(arrived.reshape(chips, half // 128, rows, 128), 1, 2)
    data = data.reshape(chips * rows, half)

    mid = capacity // 2
    gate_rows, up_rows, down_rows = w_gate[0], w_up[0], w_down[0]
    top = jnp.dot(one_hot[:mid], data, preferred_element_type=F32).astype(BF)
    bottom = jnp.dot(one_hot[mid:], data, preferred_element_type=F32).astype(BF)
    below_top = shift_y(top, 1)
    above_bottom = shift_y(bottom, -1)
    below_bottom = shift_y(bottom, 1)
    above_top = shift_y(top, -1)
    far_top = shift_y(below_top, 1)
    far_bottom = shift_y(above_bottom, -1)
    acts = gate_up(
        [top, bottom, swap_cores(top), swap_cores(bottom)],
        [(0, 0, mid), (0, mid, capacity), (1, 0, mid), (1, mid, capacity)],
        ((0, 0), (0, 1)),
        gate_rows, up_rows, None, capacity,
    )
    around = ((-1, 0), (1, 0), (-1, 1), (1, 1))
    for close, top_at, bottom_at in (
        ([below_top, above_bottom], 0, 1), ([above_top, below_bottom], 1, 0)
    ):
        acts = gate_up(
            close + [swap_cores(v) for v in close],
            [
                (top_at, 0, mid),
                (bottom_at, mid, capacity),
                (top_at + 2, 0, mid),
                (bottom_at + 2, mid, capacity),
            ],
            around,
            gate_rows, up_rows, acts, capacity,
        )
    far = [far_top, far_bottom]
    order = (2, 1, -1, 0)
    hidden, *far_parts = gate_up(
        far + [swap_cores(v) for v in far],
        [(0, 0, mid), (0, mid, capacity), (1, 0, mid), (1, mid, capacity)],
        ((2, 0), (2, 1)),
        gate_rows, up_rows, acts, capacity,
        down_rows, ((2, 1), (2, 0)),
    )
    far_peer = swap_cores(far_parts[0])
    rest = down(hidden, down_rows, tuple((off, peer) for peer in (1, 0) for off in order[1:]), half)
    parts = [far_parts[0], *rest[:3], far_parts[1], *rest[3:]]

    def add(*values):
        return sum(v.astype(F32) for v in values).astype(BF)

    def chip_sums(k, peer):
        return lax.optimization_barrier(
            (add(parts[4 + k][:mid], peer[:mid]), add(parts[4 + k][mid:], peer[mid:]))
        )

    peers = [far_peer] + [swap_cores(v) for v in rest[:3]]
    far_top, far_bottom = chip_sums(0, peers[0])
    top_in = shift_y(far_top, 1)
    bottom_in = shift_y(far_bottom, -1)
    up_top, up_bottom = chip_sums(1, peers[1])
    dn_top, dn_bottom = chip_sums(2, peers[2])
    below_bottom = shift_y(up_bottom, 1)
    above_top = shift_y(dn_top, -1)
    below_top = shift_y(lax.optimization_barrier(add(up_top, top_in)), 1)
    above_bottom = shift_y(lax.optimization_barrier(add(dn_bottom, bottom_in)), -1)
    part_own, peer_own = parts[7], peers[3]
    reduced = jnp.concatenate(
        [
            add(part_own[:mid], peer_own[:mid], below_top, above_top),
            add(part_own[mid:], peer_own[mid:], below_bottom, above_bottom),
        ]
    )

    back = lax.dot_general(
        one_hot, reduced, (((0,), (0,)), ((), ())), preferred_element_type=F32
    ).astype(BF)
    returned = lax.all_to_all(back.reshape(chips, rows, half), ("x", "z"), 0, 0, tiled=True)
    summed = jnp.sum(
        returned.reshape(EXPERTS, holders, rows, half).astype(F32), axis=1
    ).reshape(EXPERTS * rows, half)
    out_own = jnp.dot(combine, summed, precision=lax.Precision.HIGHEST).astype(BF)
    out_peer = jnp.dot(combine_peer, summed, precision=lax.Precision.HIGHEST).astype(BF)
    out_swap = swap_cores(out_peer)
    low = jnp.where(core == 0, out_own, out_swap)
    high = jnp.where(core == 0, out_swap, out_own)
    return jnp.concatenate([low, high], axis=1)


def solution(mesh):
    chips = Mesh(mesh.devices.reshape(4, 8, 2, mesh.shape["mp"]), ("x", "z", "c", "y"))
    placed = (
        P(EXPERT, "y"),
        P(EXPERT, None),
        P(EXPERT, None),
        P(EXPERT, None, "y"),
        P(EXPERT, None, "y"),
        P(EXPERT, "y", None),
    )
    return jax.shard_map(
        layer, mesh=chips, in_specs=placed, out_specs=P(EXPERT, "y"), check_vma=False
    )
```
